32 devices in a mesh: dp: 8 (over z, x), expert: 4 (over y, core).
Axes of the slice: x: 2, y: 2, z: 4, core: 2. Of those that a mesh axis runs over, the one named last changes fastest.
Arguments:
- tokens: bfloat16 [4096, 2048], P(('dp', 'expert')), may hold values from -6 to 6
- expert_ids: int32 [4096, 8], P(('dp', 'expert')), may hold values from 0 to 15, all different within a row
- route_probs: float32 [4096, 8], P(('dp', 'expert')), may hold values from 0.05 to 1
- shard_limit: int32 [32, 16], P(('dp', 'expert')), may hold values from 32 to 64
- gate_proj: bfloat16 [32, 2048, 384], P(('dp', 'expert')), may hold values from -0.125 to 0.125
- up_proj: bfloat16 [32, 2048, 384], P(('dp', 'expert')), may hold values from -0.125 to 0.125
- down_proj: bfloat16 [32, 384, 2048], P(('dp', 'expert')), may hold values from -0.21875 to 0.21875
Outputs:
- mixed_out: bfloat16 [4096, 2048], P(('dp', 'expert'))
The draws below stay inside these ranges and needn't reach their ends.
Inputs may be any that keep to these rules, and one draw needn't show every extreme that they name: `expert_ids`: each row names 8 different experts.
All inputs are finite; a program needn't handle non-finite values.
Results may differ from the reference program's by a relative error of at most 0.0095.
Values may be sent and summed in bfloat16 or wider, within the bound.
A program may use at most 64 MiB of HBM per device.

```python
import math
import jax
import jax.numpy as jnp
from jax import lax

D = 2048
FF = 768
TOP = 8
TOK_DEV = 128
EXPERTS = 16
SHARDS = 32
TOKENS = 4096
CAP = 64
COL_CAP = 256
N_DP = 8
N_EXPERT = 4


def draw_shard_limit(key, part):
    key_base = jax.random.fold_in(key, 11)
    key_full = jax.random.fold_in(key, 12)
    drawn_base = jax.random.randint(key_base, (SHARDS, EXPERTS), CAP // 2, CAP + 1)
    full_mark = jax.random.randint(key_full, (SHARDS, EXPERTS), 0, 2)
    return jnp.where(full_mark == 1, CAP, drawn_base).astype(jnp.int32)


def block_levels(key, extent, split, least, largest):
    factor_of = 1.0
    for dim, parts in split:
        heights = jax.random.uniform(jax.random.fold_in(jax.random.fold_in(key, 6), dim), (parts,), jnp.float32, least / len(split), largest / len(split))
        factor_of = factor_of * jnp.repeat(jnp.exp(heights), extent[dim] // parts).reshape((-1,) + (1,) * (len(extent) - 1 - dim))
    return factor_of


def choose_distinct(own_key, rows, number_of, top, lift):
    sequence = jax.random.permutation(jax.random.fold_in(own_key, 1), number_of)
    boost = sequence
    for power in range(3):
        boost = boost * boost // number_of
    boost = boost * lift // number_of
    lots = jax.random.randint(jax.random.fold_in(own_key, 2), (rows, number_of), 0, 4096) + boost
    sure = jax.random.permutation(jax.random.fold_in(own_key, 3), rows)[jnp.arange(number_of) % rows]
    lots = jnp.where(jnp.arange(rows)[:, None] == sure[None, :], 1 << 14, lots)
    merit = lots * number_of + jnp.arange(number_of)
    return lax.top_k(merit.astype(jnp.int32), top)[1].astype(jnp.int32)


def noise(own_key, shape, spread, most, split=(), held_as=jnp.bfloat16):
    factor_of = block_levels(own_key, shape, split, -0.22, 0.18) if split else 1.0
    values = jax.random.normal(own_key, shape, jnp.float32) * spread * factor_of
    return jnp.minimum(jnp.maximum(values, -most), most).astype(held_as)


def setup_inputs(seed: int = 0) -> dict:
    keys = jax.random.split(jax.random.key(seed), 8)
    return {
        "tokens": noise(keys[0], (TOKENS, D), 1.0, 6.0, ((0, 32),)),
        "expert_ids": choose_distinct(keys[1], TOKENS, EXPERTS, TOP, 8192),
        "route_probs": jnp.clip(jnp.exp(math.log(1.0) - 2.9957323 * jax.random.uniform(keys[2], (TOKENS, TOP), jnp.float32) ** block_levels(keys[2], (TOKENS, TOP), ((0, 32),), -0.2, 0.2)), 0.05, 1.0),
        "shard_limit": draw_shard_limit(jax.random.fold_in(keys[7], 71), 0),
        "gate_proj": noise(keys[4], (2 * EXPERTS, D, FF // 2), D ** -0.5, 0.125, ((0, 32),)),
        "up_proj": noise(keys[5], (2 * EXPERTS, D, FF // 2), D ** -0.5, 0.125, ((0, 32),)),
        "down_proj": noise(keys[6], (2 * EXPERTS, FF // 2, D), FF ** -0.5, 0.21875, ((0, 32),)),
    }


def half_pair(rows_in, gate_pair, up_pair, down_pair):
    partials = []
    for half_index in range(2):
        gate_val = jnp.dot(rows_in, gate_pair[half_index], preferred_element_type=jnp.float32)
        up_val = jnp.dot(rows_in, up_pair[half_index], preferred_element_type=jnp.float32)
        hidden = (jax.nn.silu(gate_val) * up_val).astype(jnp.bfloat16)
        partials.append(jnp.dot(hidden, down_pair[half_index], preferred_element_type=jnp.float32).astype(jnp.bfloat16))
    return (partials[0].astype(jnp.float32) + partials[1].astype(jnp.float32)).astype(jnp.bfloat16)


def expert_apply(packed):
    return half_pair(packed[0], packed[1], packed[2], packed[3])


def reference(tokens, expert_ids, route_probs, shard_limit, gate_proj, up_proj, down_proj):
    shards = N_DP * N_EXPERT
    route_ids = expert_ids.reshape(shards, TOK_DEV * TOP)
    onehot = (route_ids[:, :, None] == jnp.arange(EXPERTS, dtype=jnp.int32)[None, None, :]).astype(jnp.int32)
    before = (jnp.cumsum(onehot, axis=1) - onehot).astype(jnp.int32)
    slot_rank = jnp.sum(before * onehot, axis=2).astype(jnp.int32)
    expert_count = jnp.sum(onehot, axis=1).astype(jnp.int32)
    kept_count = jnp.minimum(expert_count, shard_limit)
    count_grid = kept_count.reshape(N_DP, N_EXPERT, EXPERTS)
    offset = (jnp.cumsum(count_grid, axis=0) - count_grid).astype(jnp.int32).reshape(shards, EXPERTS)
    limit_each = jnp.take_along_axis(shard_limit, route_ids, axis=1)
    offset_each = jnp.take_along_axis(offset, route_ids, axis=1)
    slot_global = offset_each + slot_rank
    kept_mask = (slot_rank < limit_each) & (slot_global < COL_CAP)
    column = (jnp.arange(shards, dtype=jnp.int32) % N_EXPERT)[:, None]
    per_expert = N_EXPERT * COL_CAP
    total_slots = EXPERTS * per_expert
    target = jnp.where(kept_mask, route_ids * per_expert + column * COL_CAP + slot_global, total_slots).astype(jnp.int32)
    target = target.reshape(shards * TOK_DEV, TOP)
    kept_rows = kept_mask.reshape(shards * TOK_DEV, TOP)
    buffers = jnp.zeros((total_slots, D), jnp.bfloat16)
    for choice_num in range(TOP):
        buffers = buffers.at[target[:, choice_num]].set(tokens, mode="drop")
    buffers = buffers.reshape(EXPERTS, per_expert, D)
    expert_rows = lax.map(expert_apply, (buffers, gate_proj.reshape(EXPERTS, 2, D, FF // 2), up_proj.reshape(EXPERTS, 2, D, FF // 2), down_proj.reshape(EXPERTS, 2, FF // 2, D)))
    flat_rows = expert_rows.reshape(total_slots, D)
    total = jnp.zeros((shards * TOK_DEV, D), jnp.float32)
    for choice_num in range(TOP):
        index_now = jnp.minimum(target[:, choice_num], total_slots - 1)
        fetched = flat_rows[index_now].astype(jnp.float32)
        weight = route_probs[:, choice_num] * kept_rows[:, choice_num].astype(jnp.float32)
        total = total + weight[:, None] * fetched
    return total.astype(jnp.bfloat16)
```

```python
import functools

import jax
import jax.numpy as jnp
from jax import lax
from jax.experimental import pallas as pl
from jax.experimental.pallas import tpu as pltpu
from jax.sharding import PartitionSpec as P

BF = jnp.bfloat16
F32 = jnp.float32
FAR = 4096.0
FORTH = (4, 2, 2)
BACK = (2, 4, 2)
MESH = pl.DeviceIdType.MESH


def cuts(width, shares):
    unit = width // sum(shares)
    spans, begin = [], 0
    for share in shares:
        spans.append((begin, unit * share))
        begin += unit * share
    return spans


class Wires:
    def __init__(self):
        self.sent = []

    def copy(self, src, dst, ssem, rsem, to):
        return pltpu.make_async_remote_copy(
            src_ref=src, dst_ref=dst, send_sem=ssem, recv_sem=rsem,
            device_id=to, device_id_type=MESH,
        )

    def send(self, src, dst, ssem, rsem, to, cond=None):
        def go():
            self.copy(src, dst, ssem, rsem, to).start()

        if cond is None:
            go()
        else:
            pl.when(cond)(go)
        self.sent.append((src, dst, ssem, rsem, to, cond))

    def arrive(self, dst, rsem, to):
        self.copy(dst, dst, rsem, rsem, to).wait_recv()

    def finish(self):
        sent, self.sent = self.sent, []
        for *args, cond in sent:
            moved = self.copy(*args)
            if cond is None:
                moved.wait_send()
            else:
                pl.when(cond)(moved.wait_send)


def layer_kernel(shape, tokens, ids, probs, limits, gate, up, down, out, *scratch):
    dp, rows_y, cap, share = shape
    line = dp // 2
    plane = 2 * rows_y
    count, width = tokens.shape
    half = width // 2
    ff = gate.shape[1]
    forth, back = cuts(half, FORTH), cuts(half, FORTH if share else BACK)
    nf, nb = len(forth), len(back)

    scratch = list(scratch)

    def take(n):
        got = scratch[:n]
        del scratch[:n]
        return got

    w1, w2, own_meta, meta, acc, hidden = take(6)
    tok, picked, rows_in = take(nf), take(nf), take(nf)
    sent_out, slots_in, ring_in = take(nb), take(nb), take(nb)
    part = tok if share else take(nb)
    (choose,) = take(1)
    blend = choose if share else take(1)[0]
    (m_s, m_r, w_s, w_r, w_l, x_s, up_s, dn_s, tok_r, p_s, p_r) = take(11)
    (q_s, q_r, ru_s, ru_r, rd_s, rd_r, f_s, f_r) = take(8)

    d, c = lax.axis_index("dp"), lax.axis_index("expert")
    z, x = lax.div(d, 2), lax.rem(d, 2)
    y, k = lax.div(c, 2), lax.rem(c, 2)
    here = x * rows_y + y
    across = {"dp": z * 2 + 1 - x, "expert": c}
    ahead = {"dp": lax.rem(d + 2, dp), "expert": c}
    behind = {"dp": lax.rem(d + dp - 2, dp), "expert": c}
    twin = {"dp": d, "expert": c + 1 - 2 * k}
    has_up, has_dn = z < line - 1, z > 0
    wires = Wires()

    def column_peer(s):
        return {"dp": lax.rem(d + s, dp), "expert": c}

    def plane_peer(dx, dy):
        to_x, to_y = lax.rem(x + dx, 2), lax.rem(y + dy, rows_y)
        return to_x, to_y, {"dp": z * 2 + to_x, "expert": to_y * 2 + k}

    offsets = [(dx, dy) for dy in range(rows_y) for dx in range(2) if dx or dy][::-1]

    barrier = pltpu.get_barrier_semaphore()
    peers = [column_peer(s) for s in range(1, dp)] + [twin]
    peers += [plane_peer(dx, dy)[2] for dx, dy in offsets if dy]
    for peer in peers:
        pl.semaphore_signal(barrier, inc=1, device_id=peer, device_id_type=MESH)

    local = [
        pltpu.make_async_copy(gate, w1.at[:, pl.ds(0, ff)], w_l.at[0]),
        pltpu.make_async_copy(up, w1.at[:, pl.ds(2 * ff, ff)], w_l.at[1]),
        pltpu.make_async_copy(down, w2.at[pl.ds(0, ff)], w_l.at[2]),
    ]
    for copy in local:
        copy.start()

    lane = lax.broadcasted_iota(jnp.int32, (count, count), 1)
    deep = lax.broadcasted_iota(jnp.int32, (count, count), 0)
    chosen = jnp.zeros((count, count), F32)
    weight = jnp.zeros((count, count), F32)
    for j in range(ids.shape[1]):
        match = lane == ids[:, j : j + 1]
        chosen = chosen + jnp.where(match, 1.0, 0.0)
        weight = weight + jnp.where(match, probs[:, j : j + 1], 0.0)
    lower = jnp.where(lane < deep, 1.0, 0.0).astype(BF)
    rank = jnp.dot(lower, chosen.astype(BF), preferred_element_type=F32)
    experts = limits.shape[1]
    limit = jnp.concatenate(
        [limits[...].astype(F32), jnp.zeros((1, count - experts), F32)], axis=1
    ) if experts < count else limits[...].astype(F32)
    rank = jnp.where((chosen > 0) & (rank < limit), rank, FAR)
    rank, weight = rank.T, weight.T
    for zz in range(line):
        own_meta[zz, :plane] = rank[zz * plane : (zz + 1) * plane]
        own_meta[zz, plane:] = weight[zz * plane : (zz + 1) * plane]
    meta[d] = own_meta[z]
    for j, (begin, w) in enumerate(forth):
        mine = pl.ds(pl.multiple_of(x * half + begin, 128), w)
        tok[j][pl.ds(pl.multiple_of(d * count, count), count)] = tokens[:, mine]

    pl.semaphore_wait(barrier, len(peers))

    def block(o):
        return pl.ds(pl.multiple_of(o * count, count), count)

    for s in range(1, dp):
        to = column_peer(s)
        wires.send(own_meta.at[lax.div(to["dp"], 2)], meta.at[d], m_s.at[s], m_r.at[d], to)

    def send_own(j):
        begin, w = forth[j]
        src = tokens.at[:, pl.ds(pl.multiple_of(x * half + begin, 128), w)]
        dst = tok[j].at[block(d)]
        wires.send(src, dst, up_s.at[j, d], tok_r.at[j, d], ahead, has_up)
        wires.send(src, dst, dn_s.at[j, d], tok_r.at[j, d], behind, has_dn)

    def send_cross(j):
        begin, w = forth[j]
        src = tokens.at[:, pl.ds(pl.multiple_of((1 - x) * half + begin, 128), w)]
        wires.send(src, tok[j].at[block(d)], x_s.at[j], tok_r.at[j, d], across)

    def collect(j):
        def ref(o):
            return tok[j].at[block(o)]

        o = z * 2 + 1 - x
        wires.arrive(ref(o), tok_r.at[j, o], across)
        wires.send(ref(o), ref(o), up_s.at[j, o], tok_r.at[j, o], ahead, has_up)
        wires.send(ref(o), ref(o), dn_s.at[j, o], tok_r.at[j, o], behind, has_dn)
        if j + 1 < nf:
            send_own(j + 1)
        for s in range(1, line):
            for xx in (x, 1 - x):
                low, high = z - s >= 0, z + s < line
                o = lax.max(z - s, 0) * 2 + xx

                @pl.when(low)
                def _():
                    wires.arrive(ref(o), tok_r.at[j, o], across)

                wires.send(
                    ref(o), ref(o), up_s.at[j, o], tok_r.at[j, o], ahead, low & has_up
                )
                o2 = lax.min(z + s, line - 1) * 2 + xx

                @pl.when(high)
                def _():
                    wires.arrive(ref(o2), tok_r.at[j, o2], across)

                wires.send(
                    ref(o2), ref(o2), dn_s.at[j, o2], tok_r.at[j, o2], behind, high & has_dn
                )

    send_own(0)
    for j in range(nf):
        send_cross(j)
    wires.send(gate, w1.at[:, pl.ds(ff, ff)], w_s.at[0], w_r.at[0], twin)
    wires.send(up, w1.at[:, pl.ds(3 * ff, ff)], w_s.at[1], w_r.at[1], twin)
    wires.send(down, w2.at[pl.ds(ff, ff)], w_s.at[2], w_r.at[2], twin)

    def wait_weights():
        for copy in local:
            copy.wait()
        wires.arrive(w1.at[:, pl.ds(ff, ff)], w_r.at[0], twin)
        wires.arrive(w1.at[:, pl.ds(3 * ff, ff)], w_r.at[1], twin)
        wires.arrive(w2.at[pl.ds(ff, ff)], w_r.at[2], twin)

    is_rank = lax.broadcasted_iota(jnp.int32, (2 * plane, count), 0) < plane

    def number_slots():
        for s in range(1, dp):
            o = lax.rem(d + s, dp)
            wires.arrive(meta.at[o], m_r.at[o], across)
        offset = jnp.zeros((2 * plane, 1), F32)
        for o in range(dp):
            given = meta[o]
            valid = is_rank & (given < FAR)
            slot = given + offset
            offset = offset + jnp.sum(jnp.where(valid, 1.0, 0.0), axis=1, keepdims=True)
            slot = jnp.where(valid & (slot < float(cap)), slot, FAR)
            meta[o] = jnp.where(is_rank, slot, given)

    spot = lax.broadcasted_iota(jnp.int32, (cap, count), 0).astype(F32)

    def build_choose():
        for p in range(plane):
            for o in range(dp):
                hit = spot == meta[o, p : p + 1]
                choose[p * cap : (p + 1) * cap, o * count : (o + 1) * count] = jnp.where(
                    hit, 1.0, 0.0
                ).astype(BF)

    spot_t = lax.broadcasted_iota(jnp.int32, (count, cap), 1).astype(F32)

    def weigh_choose():
        for p in range(plane):
            for o in range(dp):
                hit = spot == meta[o, p : p + 1]
                piece = jnp.where(hit, meta[o, plane + p : plane + p + 1], 0.0).astype(BF)
                choose[p * cap : (p + 1) * cap, o * count : (o + 1) * count] = piece

    def build_blend():
        deep_rows = 2 * plane
        group = count // deep_rows
        for g in range(0, dp, group):
            n = min(group, dp - g)
            value = meta[g : g + n].reshape(n * deep_rows, count)
            if n < group:
                value = jnp.concatenate(
                    [value, jnp.zeros((count - n * deep_rows, count), F32)], axis=0
                )
            value = value.T
            for i in range(n):
                o = g + i
                for p in range(plane):
                    a = i * deep_rows + p
                    hit = spot_t == value[:, a : a + 1]
                    b = a + plane
                    piece = jnp.where(hit, value[:, b : b + 1], 0.0).astype(BF)
                    blend[o * count : (o + 1) * count, p * cap : (p + 1) * cap] = piece

    def pick(j):
        begin, w = forth[j]
        for dx, dy in offsets + [(0, 0)]:
            to_x, to_y, to = plane_peer(dx, dy)
            there = to_x * rows_y + to_y
            got = jnp.dot(
                choose[pl.ds(pl.multiple_of(there * cap, cap), cap)],
                tok[j][...],
                preferred_element_type=F32,
            ).astype(BF)
            mine = pl.ds(pl.multiple_of(y * cap, cap), cap)
            if dx or dy:
                n = dx * rows_y + dy
                picked[j][n] = got
                wires.send(
                    picked[j].at[n], rows_in[j].at[x, mine], p_s.at[j, n], p_r.at[j, n], to
                )
            else:
                rows_in[j][x, mine] = got

    def expand(j):
        begin, w = forth[j]
        for dx, dy in offsets:
            n = dx * rows_y + dy
            from_x = lax.rem(x + dx, 2)
            from_y = lax.rem(y + rows_y - dy, rows_y)
            spot_in = rows_in[j].at[from_x, pl.ds(pl.multiple_of(from_y * cap, cap), cap)]
            wires.arrive(spot_in, p_r.at[j, n], across)
        for n in range(0, 4 * ff, 2 * ff):
            cols = pl.ds(n, 2 * ff)
            value = jnp.dot(rows_in[j][0], w1[begin : begin + w, cols], preferred_element_type=F32)
            value = value + jnp.dot(
                rows_in[j][1], w1[half + begin : half + begin + w, cols],
                preferred_element_type=F32,
            )
            if j == 0:
                acc[:, cols] = value
            else:
                acc[:, cols] += value

    number_slots()
    build_choose()
    for j in range(nf):
        collect(j)
        if j == 0 and not share:
            build_blend()
        pick(j)
        if j == 1:
            wait_weights()
        if j > 0:
            expand(j - 1)
    if nf == 1:
        wait_weights()
    expand(nf - 1)

    gated = acc[:, : 2 * ff]
    hidden[...] = (gated / (1.0 + jnp.exp(-gated)) * acc[:, 2 * ff :]).astype(BF)
    if share:
        wires.finish()
        weigh_choose()

    def project(j):
        begin, w = back[j]
        for dx, dy in offsets + [(0, 0)]:
            to_x, to_y, to = plane_peer(dx, dy)
            cols = pl.ds(pl.multiple_of(to_x * half + begin, 128), w)
            value = jnp.dot(
                hidden[pl.ds(pl.multiple_of(to_y * cap, cap), cap)],
                w2[:, cols],
                preferred_element_type=F32,
            ).astype(BF)
            home = pl.ds(pl.multiple_of(here * cap, cap), cap)
            if dx or dy:
                n = dx * rows_y + dy
                sent_out[j][n] = value
                wires.send(
                    sent_out[j].at[n], slots_in[j].at[home], q_s.at[j, n], q_r.at[j, n], to
                )
            else:
                slots_in[j][home] = value

    def mix(j):
        for dx, dy in offsets:
            n = dx * rows_y + dy
            from_x = lax.rem(x + dx, 2)
            from_y = lax.rem(y + rows_y - dy, rows_y)
            home = pl.ds(pl.multiple_of((from_x * rows_y + from_y) * cap, cap), cap)
            wires.arrive(slots_in[j].at[home], q_r.at[j, n], across)
        value = slots_in[j][...]
        if share:
            got = lax.dot_general(
                blend[...], value, (((0,), (0,)), ((), ())), preferred_element_type=F32
            )
        else:
            got = jnp.dot(blend[...], value, preferred_element_type=F32)
        part[j][...] = got.astype(BF)

    def pair(o):
        return pl.ds(o * 2 * count, 2 * count)

    def hop(j, o, upward, cond):
        rows = part[j].at[pair(o)]
        slot = ring_in[j].at[o + 1 if upward else o]
        ssem, rsem = (ru_s, ru_r) if upward else (rd_s, rd_r)
        wires.send(
            rows, slot, ssem.at[j, o], rsem.at[j, o], ahead if upward else behind, cond
        )

    def join(j, o, upward, cond):
        rsem = ru_r if upward else rd_r
        slot = ring_in[j].at[o + 1 if upward else o]

        @pl.when(cond)
        def _():
            wires.arrive(slot, rsem.at[j, o], across)
            part[j][pair(o)] = (part[j][pair(o)].astype(F32) + slot[...].astype(F32)).astype(BF)

    def reduce_ends(j):
        for t in range(line - 1):
            hop(j, line - 1 - t, True, z == 0)
            hop(j, t, False, z == line - 1)

    def reduce_rest(j):
        for t in range(line - 1):
            o = line - 1 - t
            cond = (z > 0) & (z < o)
            join(j, o, True, cond)
            hop(j, o, True, cond)
            cond = (z < line - 1) & (z > t)
            join(j, t, False, cond)
            hop(j, t, False, cond)

    def settle(j):
        begin, w = back[j]
        rows = pl.ds(pl.multiple_of(z * 2 * count, 2 * count), 2 * count)

        @pl.when(has_dn)
        def _():
            slot = ring_in[j].at[z + 1]
            wires.arrive(slot, ru_r.at[j, z], across)
            part[j][rows] = (part[j][rows].astype(F32) + slot[...].astype(F32)).astype(BF)

        @pl.when(has_up)
        def _():
            slot = ring_in[j].at[z]
            wires.arrive(slot, rd_r.at[j, z], across)
            part[j][rows] = (part[j][rows].astype(F32) + slot[...].astype(F32)).astype(BF)

        cols = pl.ds(pl.multiple_of(x * half + begin, 128), w)
        wires.send(
            part[j].at[block(z * 2 + 1 - x)], out.at[:, cols], f_s.at[j], f_r.at[j], across
        )
        out[:, cols] = part[j][block(d)]

    project(0)
    for j in range(nb):
        if j + 1 < nb:
            project(j + 1)
        mix(j)
        reduce_ends(j)
        if j > 0:
            reduce_rest(j - 1)
            settle(j - 1)
    reduce_rest(nb - 1)
    settle(nb - 1)
    for j, (begin, w) in enumerate(back):
        cols = pl.ds(pl.multiple_of((1 - x) * half + begin, 128), w)
        wires.arrive(out.at[:, cols], f_r.at[j], across)
    wires.finish()


def on_device(tokens, expert_ids, route_probs, shard_limit, gate_proj, up_proj, down_proj):
    count, width = tokens.shape
    top = expert_ids.shape[1]
    experts = shard_limit.shape[1]
    dp, cols = lax.axis_size("dp"), lax.axis_size("expert")
    rows_y = cols // 2
    cap = dp * (count * top // experts) // 2
    line, plane, half = dp // 2, 2 * rows_y, width // 2
    ff = gate_proj.shape[2]
    all_tok, all_slots, rows = dp * count, plane * cap, rows_y * cap
    share = all_tok * all_slots > 1 << 21
    forth, back = cuts(half, FORTH), cuts(half, FORTH if share else BACK)
    nf, nb = len(forth), len(back)
    scratch = [
        pltpu.VMEM((width, 4 * ff), BF),
        pltpu.VMEM((2 * ff, width), BF),
        pltpu.VMEM((line, 2 * plane, count), F32),
        pltpu.VMEM((dp, 2 * plane, count), F32),
        pltpu.VMEM((rows, 4 * ff), F32),
        pltpu.VMEM((rows, 2 * ff), BF),
    ]
    scratch += [pltpu.VMEM((all_tok, w), BF) for _, w in forth]
    scratch += [pltpu.VMEM((plane, cap, w), BF) for _, w in forth]
    scratch += [pltpu.VMEM((2, rows, w), BF) for _, w in forth]
    scratch += [pltpu.VMEM((plane, cap, w), BF) for _, w in back]
    scratch += [pltpu.VMEM((all_slots, w), BF) for _, w in back]
    scratch += [pltpu.VMEM((line + 1, 2 * count, w), BF) for _, w in back]
    if not share:
        scratch += [pltpu.VMEM((all_tok, w), BF) for _, w in back]
    scratch += [pltpu.VMEM((all_slots, all_tok), BF)]
    if not share:
        scratch += [pltpu.VMEM((all_tok, all_slots), BF)]
    DMA = pltpu.SemaphoreType.DMA
    scratch += [DMA((dp,)), DMA((dp,)), DMA((3,)), DMA((3,)), DMA((3,)), DMA((nf,))]
    scratch += [DMA((nf, dp)), DMA((nf, dp)), DMA((nf, dp)), DMA((nf, plane)), DMA((nf, plane))]
    scratch += [DMA((nb, plane)), DMA((nb, plane))] + [DMA((nb, line))] * 4
    scratch += [DMA((nb,)), DMA((nb,))]
    vm, anywhere = pl.BlockSpec(memory_space=pltpu.VMEM), pl.BlockSpec(memory_space=pl.ANY)
    return pl.pallas_call(
        functools.partial(layer_kernel, (dp, rows_y, cap, share)),
        name="layer",
        out_shape=jax.ShapeDtypeStruct((count, width), BF),
        in_specs=[vm] * 4 + [anywhere] * 3,
        out_specs=vm,
        scratch_shapes=scratch,
        compiler_params=pltpu.CompilerParams(
            collective_id=0, has_side_effects=True, vmem_limit_bytes=62 << 20
        ),
    )(tokens, expert_ids, route_probs, shard_limit, gate_proj[0], up_proj[0], down_proj[0])


def solution(mesh):
    rows = P(("dp", "expert"), None)
    blocks = P(("dp", "expert"), None, None)
    return jax.shard_map(
        on_device,
        mesh=mesh,
        in_specs=(rows, rows, rows, rows, blocks, blocks, blocks),
        out_specs=rows,
        check_vma=False,
    )
```
